128 devices in a mesh: bank: 4 (over z), zero: 32 (over y, x, core).
Axes of the slice: x: 4, y: 4, z: 4, core: 2. Of those that a mesh axis runs over, the one named last changes fastest.
Arguments:
- w_gate: float32 [128, 2048, 768], P('bank', 'zero'), may hold values from -0.25 to 0.25
- w_up: float32 [128, 2048, 768], P('bank', 'zero'), may hold values from -0.25 to 0.25
- router_weight: float32 [2048, 128], P('zero', 'bank'), may hold values from -0.125 to 0.125
- router_gain: float32 [2048], P('zero'), may hold values from 0.25 to 1.75
Outputs:
- serve_gate: bfloat16 [128, 2048, 768], P('bank', None, 'zero')
- serve_up: bfloat16 [128, 2048, 768], P('bank', None, 'zero')
- scale_gate: float32 [128, 768], P('bank', 'zero')
- scale_up: float32 [128, 768], P('bank', 'zero')
- serve_router: bfloat16 [2048, 128], replicated
The draws below stay inside these ranges and needn't reach their ends.
All inputs are finite; a program needn't handle non-finite values.
Results may differ from the reference program's by a relative error of at most 0.001.
Values may be sent and summed in bfloat16 or wider, within the bound.
A program may use at most 128 MiB of HBM per device.

```python
import jax
import jax.numpy as jnp
from jax import lax

EXPERTS = 128
D_MODEL = 2048
D_EXPERT = 768


def strengthened(drawn, own_key, source, target, shards_of, factor):
    owner, partner = [(jnp.arange(drawn.shape[position]) // (drawn.shape[position] // shards_of)).reshape([-1 if axis == position else 1 for axis in range(drawn.ndim)]) for position in (source, target)]
    chosen = jax.random.permutation(own_key, shards_of)[partner]
    strong = (owner == chosen) | (owner == (partner + shards_of // 2) % shards_of)
    return jnp.where(strong, factor * drawn, drawn)


def block_levels(key, shape, shards, least, top_value):
    gain, own = 1.0, jax.random.fold_in(key, 6)
    for dim, blocks in shards:
        steps = jnp.exp(jax.random.uniform(jax.random.fold_in(own, dim), (blocks,), jnp.float32, least / len(shards), top_value / len(shards)))
        gain = gain * jnp.repeat(steps, shape[dim] // blocks).reshape([-1 if axis == dim else 1 for axis in range(len(shape))])
    return gain


def noise(stream_key, shape, spread, limit, cuts=(), dtype=jnp.bfloat16):
    result = jax.random.normal(stream_key, shape, jnp.float32) * spread
    if len(cuts) > 0:
        result = block_levels(stream_key, shape, cuts, -0.22, 0.18) * result
    return jnp.clip(result, min=-limit, max=limit).astype(dtype)


def bell_draw_with(key, extent, scale, limit, shards, heavy, held_as=jnp.bfloat16):
    drawn = scale * jax.random.normal(key, extent, jnp.float32)
    if shards:
        drawn = drawn * block_levels(key, extent, shards, -0.22, 0.18)
    return jnp.clip(strengthened(drawn, jax.random.fold_in(key, 3), *heavy), -limit, limit).astype(held_as)


def setup_inputs(seed: int = 0) -> dict:
    streams_of = jax.random.split(jax.random.key(seed), 5)
    return {
        "w_gate": bell_draw_with(streams_of[0], (EXPERTS, D_MODEL, D_EXPERT), D_MODEL ** -0.5, 0.25, ((0, 4), (1, 32)), (1, 2, 32, 2.75), jnp.float32),
        "w_up": bell_draw_with(streams_of[1], (EXPERTS, D_MODEL, D_EXPERT), D_MODEL ** -0.5, 0.25, ((0, 4), (1, 32)), (1, 2, 32, 2.75), jnp.float32),
        "router_weight": noise(streams_of[2], (D_MODEL, EXPERTS), D_MODEL ** -0.5, 0.125, ((0, 32), (1, 4)), jnp.float32),
        "router_gain": jnp.clip(1.0 + 0.15 * jax.random.normal(streams_of[3], (D_MODEL,), jnp.float32), 0.25, 1.75),
    }


def reference(w_gate, w_up, router_weight, router_gain):
    scale_gate = jnp.sqrt(lax.optimization_barrier(jnp.sum(w_gate * w_gate, axis=1)))
    serve_gate = (w_gate / jnp.expand_dims(scale_gate, 1)).astype(jnp.bfloat16)
    scale_up = jnp.sqrt(lax.optimization_barrier(jnp.sum(w_up * w_up, axis=1)))
    serve_up = (w_up / jnp.expand_dims(scale_up, 1)).astype(jnp.bfloat16)
    serve_router = (router_weight * router_gain[:, None]).astype(jnp.bfloat16)
    return (serve_gate, serve_up, scale_gate, scale_up, serve_router)
```

```python
import functools

import jax
import jax.numpy as jnp
from jax import lax
from jax.experimental import pallas as pl
from jax.experimental.pallas import tpu as pltpu
from jax.sharding import PartitionSpec as P

MESH = pl.DeviceIdType.MESH
Z = 32
LANES = 128


def plane_peer(me, k):
    k = (11 * k) % 32
    dy, dx, dc = k // 8, (k // 2) % 4, k % 2
    y, x, c = me // 8, (me // 2) % 4, me % 2
    return (((y + dy) % 4) * 4 + (x + dx) % 4) * 2 + (c + dc) % 2


def exchange(
    experts, rows, cols, chunk,
    gate_hbm, up_hbm, router_ref, gain_ref,
    out_gate, out_up, out_sgate, out_sup, out_router,
    held, sums, parts, scales, inverse, scales_t, send, recv, router_part, router_got,
    load_sem, rs_send, rs_recv, ag_send, ag_recv, bulk_send, bulk_recv,
    rt_send, rt_recv, rx_send, rx_recv,
):
    bank = lax.axis_index("bank")
    me = lax.axis_index("zero")
    core = me % 2
    blocks = cols // LANES
    own = cols // Z
    pairs = experts // 2
    half = blocks // 2
    weights = (gate_hbm, up_hbm)
    loads = 4
    step = experts // loads

    barrier = pltpu.get_barrier_semaphore()

    def greet(k, _):
        pl.semaphore_signal(barrier, inc=1, device_id={"zero": plane_peer(me, k)}, device_id_type=MESH)
        return 0

    lax.fori_loop(1, Z, greet, 0)
    for dz in range(1, 4):
        for dc in range(2):
            pl.semaphore_signal(
                barrier, inc=1,
                device_id={"bank": (bank + dz) % 4, "zero": (me // 2) * 2 + (core + dc) % 2},
                device_id_type=MESH,
            )

    copies = []
    for w in range(2):
        for q in range(loads):
            at = pl.ds(q * step, step)
            copy = pltpu.make_async_copy(weights[w].at[at], held.at[w, at], load_sem.at[w * loads + q])
            copy.start()
            copies.append(copy)

    low = router_ref[:16, :] * gain_ref[...]
    high = router_ref[16:, :] * gain_ref[...]
    first = jnp.where(core == 0, low, high)
    second = jnp.where(core == 0, high, low)
    packed = jnp.concatenate([first, second], axis=1).astype(jnp.bfloat16)
    router_part[me // 2] = packed

    def sums_of(w, q):
        copies[w * loads + q].wait()

        def body(e, _):
            for b in range(blocks):
                x = held[w, e, :, b * LANES:(b + 1) * LANES]
                sums[w, e, b:b + 1, :] = jnp.sum(x * x, axis=0, keepdims=True)
            return 0

        lax.fori_loop(q * step, (q + 1) * step, body, 0)

    def to_plane(make):
        def body(k, _):
            make(plane_peer(me, k)).start()
            return 0

        lax.fori_loop(1, Z, body, 0)

    def scatter_sums(w):
        to_plane(lambda t: pltpu.make_async_remote_copy(
            src_ref=sums.at[w, t], dst_ref=parts.at[w, me], send_sem=rs_send.at[w], recv_sem=rs_recv.at[w],
            device_id={"zero": t}, device_id_type=MESH))
        parts[w, me] = sums[w, me]

    def gather_scales(w):
        got = parts.at[w, pl.ds(0, Z - 1)]
        pltpu.make_async_copy(got, got, rs_recv.at[w]).wait()
        scales[w, me] = jnp.sqrt(jnp.sum(parts[w], axis=0))
        to_plane(lambda t: pltpu.make_async_remote_copy(
            src_ref=scales.at[w, me], dst_ref=scales.at[w, me], send_sem=ag_send.at[w], recv_sem=ag_recv.at[w],
            device_id={"zero": t}, device_id_type=MESH))

    def finish_scales(w):
        got = scales.at[w, pl.ds(0, Z - 1)]
        pltpu.make_async_copy(got, got, ag_recv.at[w]).wait()
        inverse[w] = 1.0 / scales[w]

    def narrow(w, p):
        e0 = 2 * p + core
        e1 = 2 * p + 1 - core
        for h in range(2):
            turned = []
            for b in range(h * half, (h + 1) * half):
                at = slice(b * LANES, (b + 1) * LANES)
                x0 = held[w, e0, :, at] * inverse[w, e0, b:b + 1, :]
                x1 = held[w, e1, :, at] * inverse[w, e1, b:b + 1, :]
                turned.append(jnp.concatenate([x0, x1], axis=0).T)
            t = jnp.concatenate(turned, axis=0).reshape(Z // 2, own, LANES).astype(jnp.bfloat16)
            send[pl.ds(h * (Z // 2), Z // 2), w * pairs + p] = t

    def send_chunk(ch):
        at = pl.ds(ch * chunk, chunk)
        to_plane(lambda t: pltpu.make_async_remote_copy(
            src_ref=send.at[t, at], dst_ref=recv.at[me, at], send_sem=bulk_send, recv_sem=bulk_recv.at[ch],
            device_id={"zero": t}, device_id_type=MESH))
        recv[me, at] = send[me, at]

    for q in range(loads):
        sums_of(0, q)
    pl.semaphore_wait(barrier, Z - 1 + 6)
    scatter_sums(0)
    for q in range(loads):
        sums_of(1, q)
    scatter_sums(1)

    def router_row(k, _):
        t = (((me // 8 + k // 4) % 4) * 4 + (me // 2 + k) % 4) * 2 + core
        pltpu.make_async_remote_copy(
            src_ref=router_part.at[me // 2], dst_ref=router_part.at[me // 2],
            send_sem=rt_send, recv_sem=rt_recv, device_id={"zero": t}, device_id_type=MESH).start()
        return 0

    gather_scales(0)
    gather_scales(1)
    lax.fori_loop(1, 16, router_row, 0)

    per_weight = pairs // chunk
    for w in range(2):
        finish_scales(w)

        def out(i, _):
            def one(p, _):
                narrow(w, p)
                return 0

            lax.fori_loop(i * chunk, (i + 1) * chunk, one, 0)
            send_chunk(w * per_weight + i)
            return 0

        lax.fori_loop(0, per_weight, out, 0)

    got = router_part.at[pl.ds(0, 15)]
    pltpu.make_async_copy(got, got, rt_recv).wait()
    router_got[2 * bank + core] = router_part[...]
    for dz in range(4):
        for dc in range(2):
            if dz or dc:
                pltpu.make_async_remote_copy(
                    src_ref=router_part, dst_ref=router_got.at[2 * bank + core], send_sem=rx_send, recv_sem=rx_recv,
                    device_id={"bank": (bank + dz) % 4, "zero": (me // 2) * 2 + (core + dc) % 2},
                    device_id_type=MESH).start()

    for w, o in ((0, out_sgate), (1, out_sup)):
        for b in range(blocks):
            scales_t[b * LANES:(b + 1) * LANES, :] = scales[w, :, b, :].T
        o[...] = scales_t[pl.ds(pl.multiple_of(me * own, 8), own), :]

    low_lanes = lax.broadcasted_iota(jnp.int32, (own, LANES), 1) < LANES // 2

    def join(ch):
        at = pl.ds(ch * chunk, chunk)
        got = recv.at[pl.ds(0, Z - 1), at]
        pltpu.make_async_copy(got, got, bulk_recv.at[ch]).wait()

    def merge(out, g, p):
        for k in range(Z // 2):
            a = recv[2 * k, g].astype(jnp.float32)
            b = recv[2 * k + 1, g].astype(jnp.float32)
            at = slice(k * LANES, (k + 1) * LANES)
            out[2 * p, :, at] = jnp.where(low_lanes, a, b).astype(jnp.bfloat16)
            out[2 * p + 1, :, at] = pltpu.roll(jnp.where(low_lanes, b, a), LANES // 2, 1).astype(jnp.bfloat16)

    def take(w, out):
        def body(i, _):
            join(w * per_weight + i)

            def one(p, _):
                merge(out, w * pairs + p, p)
                return 0

            lax.fori_loop(i * chunk, (i + 1) * chunk, one, 0)
            return 0

        lax.fori_loop(0, per_weight, body, 0)

    take(0, out_gate)

    got = router_got.at[pl.ds(0, 7)]
    pltpu.make_async_copy(got, got, rx_recv).wait()
    low_r = lax.broadcasted_iota(jnp.int32, (16, LANES), 1) < LANES // 2

    def router_rows(k, _):
        pieces = []
        for z in range(4):
            a = router_got[2 * z, k].astype(jnp.float32)
            b = router_got[2 * z + 1, k].astype(jnp.float32)
            pieces.append(jnp.where(low_r, a, b))
            pieces.append(pltpu.roll(jnp.where(low_r, b, a), LANES // 2, 1))
        out_router[pl.ds(pl.multiple_of(k * LANES, LANES), LANES), :] = (
            jnp.concatenate(pieces, axis=0).T.astype(jnp.bfloat16))
        return 0

    lax.fori_loop(0, 16, router_rows, 0)

    take(1, out_up)

    for w in range(2):
        left = sums.at[w, pl.ds(0, Z - 1)]
        pltpu.make_async_copy(left, left, rs_send.at[w]).wait()
        pltpu.make_async_copy(left, left, ag_send.at[w]).wait()
    left = send.at[pl.ds(0, Z - 1)]
    pltpu.make_async_copy(left, left, bulk_send).wait()
    left = router_part.at[pl.ds(0, 15)]
    pltpu.make_async_copy(left, left, rt_send).wait()
    left = router_got.at[pl.ds(0, 7)]
    pltpu.make_async_copy(left, left, rx_send).wait()


def write_out(*refs):
    n = 5
    ins, outs, sem = refs[:n], refs[n:2 * n], refs[2 * n]
    copies = []
    for i in range(n):
        copy = pltpu.make_async_copy(ins[i], outs[i], sem.at[i])
        copy.start()
        copies.append(copy)
    for copy in copies:
        copy.wait()


def shards(w_gate, w_up, router_weight, router_gain):
    experts, rows, cols = w_gate.shape
    own = cols // Z
    chunk = 4
    pairs = experts // 2
    chunks = 2 * pairs // chunk
    f32, bf16 = jnp.float32, jnp.bfloat16
    dma = pltpu.SemaphoreType.DMA
    hbm = pl.BlockSpec(memory_space=pltpu.HBM)
    vmem = pl.BlockSpec(memory_space=pltpu.VMEM)
    shapes = [
        ((experts, own, Z * rows), bf16), ((experts, own, Z * rows), bf16),
        ((own, experts), f32), ((own, experts), f32), ((Z * rows, LANES), bf16),
    ]
    moved = pl.pallas_call(
        functools.partial(exchange, experts, rows, cols, chunk),
        out_shape=[pltpu.VMEM(s, d) for s, d in shapes],
        in_specs=[hbm, hbm, vmem, vmem],
        out_specs=[vmem] * 5,
        scratch_shapes=[
            pltpu.VMEM((2, experts, rows, cols), f32),
            pltpu.VMEM((2, experts, cols // LANES, LANES), f32),
            pltpu.VMEM((2, Z, cols // LANES, LANES), f32),
            pltpu.VMEM((2, experts, cols // LANES, LANES), f32),
            pltpu.VMEM((2, experts, cols // LANES, LANES), f32),
            pltpu.VMEM((cols, experts), f32),
            pltpu.VMEM((Z, 2 * pairs, own, LANES), bf16),
            pltpu.VMEM((Z, 2 * pairs, own, LANES), bf16),
            pltpu.VMEM((16, 16, LANES), bf16),
            pltpu.VMEM((8, 16, 16, LANES), bf16),
            dma((8,)), dma((2,)), dma((2,)), dma((2,)), dma((2,)), dma, dma((chunks,)),
            dma, dma, dma, dma,
        ],
        compiler_params=pltpu.CompilerParams(
            collective_id=0, has_side_effects=True, vmem_limit_bytes=54 << 20),
    )(w_gate, w_up, router_weight.T, router_gain[None, :])
    outs = pl.pallas_call(
        write_out,
        out_shape=[jax.ShapeDtypeStruct(s, d) for s, d in shapes],
        in_specs=[pl.BlockSpec(memory_space=pl.ANY)] * 5,
        out_specs=[hbm] * 5,
        scratch_shapes=[dma((5,))],
        compiler_params=pltpu.CompilerParams(vmem_limit_bytes=1 << 20),
    )(*moved)
    gate, up, sgate, sup, router = outs
    return (gate.transpose(0, 2, 1), up.transpose(0, 2, 1), sgate.T, sup.T, router)


def solution(mesh):
    placed = (P("bank", "zero", None), P("bank", "zero", None), P("zero", "bank"), P("zero"))
    return jax.shard_map(
        shards,
        mesh=mesh,
        in_specs=placed,
        out_specs=(
            P("bank", None, "zero"),
            P("bank", None, "zero"),
            P("bank", "zero"),
            P("bank", "zero"),
            P(),
        ),
        check_vma=False,
    )
```

```python
import functools

import jax
import jax.numpy as jnp
from jax import lax
from jax.experimental import pallas as pl
from jax.experimental.pallas import tpu as pltpu
from jax.sharding import PartitionSpec as P

MESH = pl.DeviceIdType.MESH
Z = 32
LANES = 128


STEPS = sorted(
    ((dy, dx, dc) for dy in range(4) for dx in range(4) for dc in range(2) if dy or dx or dc),
    key=lambda s: -(min(s[0], 4 - s[0]) + min(s[1], 4 - s[1])),
)


def stepped(me, step):
    y, x, c = me // 8, (me // 2) % 4, me % 2
    return (((y + step[0]) % 4) * 4 + (x + step[1]) % 4) * 2 + (c + step[2]) % 2


def plane_peer(me, k):
    k = (11 * k) % 32
    dy, dx, dc = k // 8, (k // 2) % 4, k % 2
    y, x, c = me // 8, (me // 2) % 4, me % 2
    return (((y + dy) % 4) * 4 + (x + dx) % 4) * 2 + (c + dc) % 2


def exchange(
    experts, rows, cols, raw, chunk,
    gate_hbm, up_hbm, router_hbm, gain_hbm,
    out_gate, out_up, out_sgate, out_sup, out_router,
    held, sums, parts, scales, inverse, scales_t, send, recv, raw_send, raw_recv, router_ref, gain_ref, router_part, router_got,
    small_sem, load_sem, rs_send, rs_recv, ag_send, ag_recv, bulk_sent, bulk_got,
    raw_sent, raw_got,
    rt_send, rt_recv, rx_send, rx_recv,
):
    bank = lax.axis_index("bank")
    me = lax.axis_index("zero")
    core = me % 2
    blocks = cols // LANES
    own = cols // Z
    pairs = experts // 2
    half = blocks // 2
    weights = (gate_hbm, up_hbm)
    loads = 4
    step = experts // loads

    def load(w, q):
        at = pl.ds(q * step, step)
        return pltpu.make_async_copy(weights[w].at[at], held.at[w, at], load_sem.at[w * loads + q])

    for q in range(loads):
        load(0, q).start()
    small = [
        pltpu.make_async_copy(router_hbm, router_ref, small_sem.at[0]),
        pltpu.make_async_copy(gain_hbm, gain_ref, small_sem.at[1]),
    ]
    for copy in small:
        copy.start()

    barrier = pltpu.get_barrier_semaphore()

    def greet(k, _):
        pl.semaphore_signal(barrier, inc=1, device_id={"zero": plane_peer(me, k)}, device_id_type=MESH)
        return 0

    lax.fori_loop(1, Z, greet, 0)
    for dz in range(1, 4):
        for dc in range(2):
            pl.semaphore_signal(
                barrier, inc=1,
                device_id={"bank": (bank + dz) % 4, "zero": (me // 2) * 2 + (core + dc) % 2},
                device_id_type=MESH,
            )

    def sums_of(w, q):
        load(w, q).wait()

        def body(e, _):
            for b in range(blocks):
                x = held[w, e, :, b * LANES:(b + 1) * LANES]
                sums[w, e, b:b + 1, :] = jnp.sum(x * x, axis=0, keepdims=True)
            return 0

        lax.fori_loop(q * step, (q + 1) * step, body, 0)

    def to_plane(make):
        for s in STEPS:
            make(stepped(me, s)).start()

    def scatter_sums(w):
        to_plane(lambda t: pltpu.make_async_remote_copy(
            src_ref=sums.at[w, t], dst_ref=parts.at[w, me], send_sem=rs_send.at[w], recv_sem=rs_recv.at[w],
            device_id={"zero": t}, device_id_type=MESH))
        parts[w, me] = sums[w, me]

    def gather_scales(w):
        got = parts.at[w, pl.ds(0, Z - 1)]
        pltpu.make_async_copy(got, got, rs_recv.at[w]).wait()
        scales[w, me] = jnp.sqrt(jnp.sum(parts[w], axis=0))
        to_plane(lambda t: pltpu.make_async_remote_copy(
            src_ref=scales.at[w, me], dst_ref=scales.at[w, me], send_sem=ag_send.at[w], recv_sem=ag_recv.at[w],
            device_id={"zero": t}, device_id_type=MESH))

    def finish_scales(w):
        got = scales.at[w, pl.ds(0, Z - 1)]
        pltpu.make_async_copy(got, got, ag_recv.at[w]).wait()
        inverse[w] = 1.0 / scales[w]

    def turn(p, piece):
        for h in range(2):
            turned = []
            for b in range(h * half, (h + 1) * half):
                both = [piece(e, b) for e in (2 * p + core, 2 * p + 1 - core)]
                turned.append(jnp.concatenate(both, axis=0).T)
            yield h, jnp.concatenate(turned, axis=0).reshape(Z // 2, own, LANES)

    def narrow(w, p):
        def piece(e, b):
            return held[w, e, :, b * LANES:(b + 1) * LANES] * inverse[w, e, b:b + 1, :]

        for h, t in turn(p, piece):
            send[pl.ds(h * (Z // 2), Z // 2), w * pairs + p] = t.astype(jnp.bfloat16)

    def copy_raw(p):
        for h, t in turn(p, lambda e, b: held[0, e, :, b * LANES:(b + 1) * LANES]):
            raw_send[p, pl.ds(h * (Z // 2), Z // 2)] = t

    def send_raw(p):
        to_plane(lambda t: pltpu.make_async_remote_copy(
            src_ref=raw_send.at[p, t], dst_ref=raw_recv.at[p, me], send_sem=raw_sent.at[p], recv_sem=raw_got.at[p],
            device_id={"zero": t}, device_id_type=MESH))
        raw_recv[p, me] = raw_send[p, me]

    first_pair = (raw, 0)
    base = (0, (pairs - raw) // chunk[0])

    def span(w, i):
        return first_pair[w] + i * chunk[w]

    def count(w):
        return (pairs - first_pair[w]) // chunk[w]

    def send_chunk(w, i):
        at = pl.ds(w * pairs + span(w, i), chunk[w])
        for s in STEPS:
            t = stepped(me, s)
            pltpu.make_async_remote_copy(
                src_ref=send.at[t, at], dst_ref=recv.at[me, at], send_sem=bulk_sent, recv_sem=bulk_got.at[base[w] + i],
                device_id={"zero": t}, device_id_type=MESH).start()
        recv[me, at] = send[me, at]

    for q in range(loads):
        load(1, q).start()
        sums_of(0, q)
    for p in range(raw):
        copy_raw(p)
    pl.semaphore_wait(barrier, Z - 1 + 6)
    scatter_sums(0)

    for copy in small:
        copy.wait()
    low = router_ref[:16, :] * gain_ref[...]
    high = router_ref[16:, :] * gain_ref[...]
    first = jnp.where(core == 0, low, high)
    second = jnp.where(core == 0, high, low)
    router_part[me // 2] = jnp.concatenate([first, second], axis=1).astype(jnp.bfloat16)

    def router_row(k, _):
        t = (((me // 8 + k // 4) % 4) * 4 + (me // 2 + k) % 4) * 2 + core
        pltpu.make_async_remote_copy(
            src_ref=router_part.at[me // 2], dst_ref=router_part.at[me // 2],
            send_sem=rt_send, recv_sem=rt_recv, device_id={"zero": t}, device_id_type=MESH).start()
        return 0

    lax.fori_loop(1, 16, router_row, 0)

    for q in range(loads):
        sums_of(1, q)
    scatter_sums(1)
    gather_scales(0)
    for p in range(raw):
        send_raw(p)
    gather_scales(1)

    for w in range(2):
        finish_scales(w)

        def out(i, _):
            for j in range(chunk[w]):
                narrow(w, span(w, i) + j)
            send_chunk(w, i)
            return 0

        lax.fori_loop(0, count(w), out, 0)

    got = router_part.at[pl.ds(0, 15)]
    pltpu.make_async_copy(got, got, rt_recv).wait()
    router_got[2 * bank + core] = router_part[...]
    for dz in range(4):
        for dc in range(2):
            if dz or dc:
                pltpu.make_async_remote_copy(
                    src_ref=router_part, dst_ref=router_got.at[2 * bank + core], send_sem=rx_send, recv_sem=rx_recv,
                    device_id={"bank": (bank + dz) % 4, "zero": (me // 2) * 2 + (core + dc) % 2},
                    device_id_type=MESH).start()

    for w, o in ((0, out_sgate), (1, out_sup)):
        for b in range(blocks):
            scales_t[b * LANES:(b + 1) * LANES, :] = scales[w, :, b, :].T
        o[...] = scales_t[pl.ds(pl.multiple_of(me * own, 8), own), :]

    low_lanes = lax.broadcasted_iota(jnp.int32, (own, LANES), 1) < LANES // 2

    def merge(out, g, p):
        for k in range(Z // 2):
            a = recv[2 * k, g].astype(jnp.float32)
            b = recv[2 * k + 1, g].astype(jnp.float32)
            at = slice(k * LANES, (k + 1) * LANES)
            out[2 * p, :, at] = jnp.where(low_lanes, a, b).astype(jnp.bfloat16)
            out[2 * p + 1, :, at] = pltpu.roll(jnp.where(low_lanes, b, a), LANES // 2, 1).astype(jnp.bfloat16)

    def take(w, out):
        def body(i, _):
            got = recv.at[pl.ds(0, Z - 1), pl.ds(w * pairs + span(w, i), chunk[w])]
            pltpu.make_async_copy(got, got, bulk_got.at[base[w] + i]).wait()
            for j in range(chunk[w]):
                merge(out, w * pairs + span(w, i) + j, span(w, i) + j)
            return 0

        lax.fori_loop(0, count(w), body, 0)

    for p in range(raw):
        got = raw_recv.at[p, pl.ds(0, Z - 1)]
        pltpu.make_async_copy(got, got, raw_got.at[p]).wait()
        even = 1.0 / out_sgate[:, 2 * p:2 * p + 1]
        odd = 1.0 / out_sgate[:, 2 * p + 1:2 * p + 2]
        for k in range(Z // 2):
            a = raw_recv[p, 2 * k]
            b = raw_recv[p, 2 * k + 1]
            at = slice(k * LANES, (k + 1) * LANES)
            out_gate[2 * p, :, at] = (jnp.where(low_lanes, a, b) * even).astype(jnp.bfloat16)
            out_gate[2 * p + 1, :, at] = (
                pltpu.roll(jnp.where(low_lanes, b, a), LANES // 2, 1) * odd).astype(jnp.bfloat16)

    take(0, out_gate)

    got = router_got.at[pl.ds(0, 7)]
    pltpu.make_async_copy(got, got, rx_recv).wait()
    low_r = lax.broadcasted_iota(jnp.int32, (16, LANES), 1) < LANES // 2

    def router_rows(k, _):
        pieces = []
        for z in range(4):
            a = router_got[2 * z, k].astype(jnp.float32)
            b = router_got[2 * z + 1, k].astype(jnp.float32)
            pieces.append(jnp.where(low_r, a, b))
            pieces.append(pltpu.roll(jnp.where(low_r, b, a), LANES // 2, 1))
        out_router[pl.ds(pl.multiple_of(k * LANES, LANES), LANES), :] = (
            jnp.concatenate(pieces, axis=0).T.astype(jnp.bfloat16))
        return 0

    lax.fori_loop(0, 16, router_rows, 0)

    take(1, out_up)

    for w in range(2):
        left = sums.at[w, pl.ds(0, Z - 1)]
        pltpu.make_async_copy(left, left, rs_send.at[w]).wait()
        pltpu.make_async_copy(left, left, ag_send.at[w]).wait()
    for p in range(raw):
        left = raw_send.at[p, pl.ds(0, Z - 1)]
        pltpu.make_async_copy(left, left, raw_sent.at[p]).wait()
    left = send.at[pl.ds(0, Z - 1), pl.ds(raw, 2 * pairs - raw)]
    pltpu.make_async_copy(left, left, bulk_sent).wait()
    left = router_part.at[pl.ds(0, 15)]
    pltpu.make_async_copy(left, left, rt_send).wait()
    left = router_got.at[pl.ds(0, 7)]
    pltpu.make_async_copy(left, left, rx_send).wait()


def write_out(*refs):
    n = 5
    ins, outs, sem = refs[:n], refs[n:2 * n], refs[2 * n]
    copies = []
    for i in range(n):
        copy = pltpu.make_async_copy(ins[i], outs[i], sem.at[i])
        copy.start()
        copies.append(copy)
    for copy in copies:
        copy.wait()


def shards(w_gate, w_up, router_weight, router_gain):
    experts, rows, cols = w_gate.shape
    own = cols // Z
    raw = 1
    chunk = (1, 1)
    pairs = experts // 2
    chunks = (pairs - raw) // chunk[0] + pairs // chunk[1]
    f32, bf16 = jnp.float32, jnp.bfloat16
    dma = pltpu.SemaphoreType.DMA
    hbm = pl.BlockSpec(memory_space=pltpu.HBM)
    vmem = pl.BlockSpec(memory_space=pltpu.VMEM)
    shapes = [
        ((experts, own, Z * rows), bf16), ((experts, own, Z * rows), bf16),
        ((own, experts), f32), ((own, experts), f32), ((Z * rows, LANES), bf16),
    ]
    moved = pl.pallas_call(
        functools.partial(exchange, experts, rows, cols, raw, chunk),
        out_shape=[pltpu.VMEM(s, d) for s, d in shapes],
        in_specs=[hbm] * 4,
        out_specs=[vmem] * 5,
        scratch_shapes=[
            pltpu.VMEM((2, experts, rows, cols), f32),
            pltpu.VMEM((2, experts, cols // LANES, LANES), f32),
            pltpu.VMEM((2, Z, cols // LANES, LANES), f32),
            pltpu.VMEM((2, experts, cols // LANES, LANES), f32),
            pltpu.VMEM((2, experts, cols // LANES, LANES), f32),
            pltpu.VMEM((cols, experts), f32),
            pltpu.VMEM((Z, 2 * pairs, own, LANES), bf16),
            pltpu.VMEM((Z, 2 * pairs, own, LANES), bf16),
            pltpu.VMEM((raw, Z, own, LANES), f32),
            pltpu.VMEM((raw, Z, own, LANES), f32),
            pltpu.VMEM((experts, rows), f32),
            pltpu.VMEM((1, rows), f32),
            pltpu.VMEM((16, 16, LANES), bf16),
            pltpu.VMEM((8, 16, 16, LANES), bf16),
            dma((2,)), dma((8,)), dma((2,)), dma((2,)), dma((2,)), dma((2,)), dma, dma((chunks,)),
            dma((raw,)), dma((raw,)),
            dma, dma, dma, dma,
        ],
        compiler_params=pltpu.CompilerParams(
            collective_id=0, has_side_effects=True, vmem_limit_bytes=54 << 20),
    )(w_gate, w_up, router_weight.T, router_gain[None, :])
    outs = pl.pallas_call(
        write_out,
        out_shape=[jax.ShapeDtypeStruct(s, d) for s, d in shapes],
        in_specs=[pl.BlockSpec(memory_space=pl.ANY)] * 5,
        out_specs=[hbm] * 5,
        scratch_shapes=[dma((5,))],
        compiler_params=pltpu.CompilerParams(vmem_limit_bytes=1 << 20),
    )(*moved)
    gate, up, sgate, sup, router = outs
    return (gate.transpose(0, 2, 1), up.transpose(0, 2, 1), sgate.T, sup.T, router)


def solution(mesh):
    placed = (P("bank", "zero", None), P("bank", "zero", None), P("zero", "bank"), P("zero"))
    return jax.shard_map(
        shards,
        mesh=mesh,
        in_specs=placed,
        out_specs=(
            P("bank", None, "zero"),
            P("bank", None, "zero"),
            P("bank", "zero"),
            P("bank", "zero"),
            P(),
        ),
        check_vma=False,
    )
```

```python
import functools

import jax
import jax.numpy as jnp
from jax import lax
from jax.experimental import pallas as pl
from jax.experimental.pallas import tpu as pltpu
from jax.sharding import PartitionSpec as P

MESH = pl.DeviceIdType.MESH
Z = 32
LANES = 128


STEPS = sorted(
    ((dy, dx, dc) for dy in range(4) for dx in range(4) for dc in range(2) if dy or dx or dc),
    key=lambda s: -(min(s[0], 4 - s[0]) + min(s[1], 4 - s[1])),
)


FAR = 22


def stepped(me, step):
    y, x, c = me // 8, (me // 2) % 4, me % 2
    return (((y + step[0]) % 4) * 4 + (x + step[1]) % 4) * 2 + (c + step[2]) % 2


def exchange(
    experts, rows, cols, tiles, chunk,
    gate_hbm, up_hbm, router_hbm, gain_hbm,
    out_gate, out_up, out_sgate, out_sup, out_router,
    held, sums, parts, scales, inverse, scales_t, send, recv, raw_send, raw_recv, router_ref, gain_ref, router_part, router_got,
    small_sem, load_sem, rs_send, rs_recv, ag_send, ag_recv, bulk_sent, bulk_got,
    raw_sent, raw_got, rest_sent, rest_got,
    rt_send, rt_recv, rx_send, rx_recv,
):
    bank = lax.axis_index("bank")
    me = lax.axis_index("zero")
    core = me % 2
    blocks = cols // LANES
    own = cols // Z
    pairs = experts // 2
    half = blocks // 2
    per_pair = own // 8
    raw = -(-sum(tiles) // per_pair)
    kept = own - 8 * (sum(tiles) - (raw - 1) * per_pair)
    weights = (gate_hbm, up_hbm)
    loads = 4
    step = experts // loads

    def load(w, q):
        at = pl.ds(q * step, step)
        return pltpu.make_async_copy(weights[w].at[at], held.at[w, at], load_sem.at[w * loads + q])

    barrier = pltpu.get_barrier_semaphore()
    for s in STEPS:
        pl.semaphore_signal(barrier, inc=1, device_id={"zero": stepped(me, s)}, device_id_type=MESH)
    up_bank, down_bank = (bank + 1) % 4, (bank + 3) % 4
    for other in (up_bank, down_bank):
        pl.semaphore_signal(barrier, inc=1, device_id={"bank": other}, device_id_type=MESH)

    for q in range(loads):
        load(0, q).start()
    small = [
        pltpu.make_async_copy(router_hbm, router_ref, small_sem.at[0]),
        pltpu.make_async_copy(gain_hbm, gain_ref, small_sem.at[1]),
    ]
    for copy in small:
        copy.start()

    def sums_of(w, q):
        load(w, q).wait()

        def body(e, _):
            for b in range(blocks):
                x = held[w, e, :, b * LANES:(b + 1) * LANES]
                sums[w, e, b:b + 1, :] = jnp.sum(x * x, axis=0, keepdims=True)
            return 0

        lax.fori_loop(q * step, (q + 1) * step, body, 0)

    def to_plane(make):
        for s in STEPS:
            make(stepped(me, s)).start()

    def scatter_sums(w):
        to_plane(lambda t: pltpu.make_async_remote_copy(
            src_ref=sums.at[w, t], dst_ref=parts.at[w, me], send_sem=rs_send.at[w], recv_sem=rs_recv.at[w],
            device_id={"zero": t}, device_id_type=MESH))
        parts[w, me] = sums[w, me]

    def gather_scales(w):
        got = parts.at[w, pl.ds(0, Z - 1)]
        pltpu.make_async_copy(got, got, rs_recv.at[w]).wait()
        scales[w, me] = jnp.sqrt(jnp.sum(parts[w], axis=0))
        to_plane(lambda t: pltpu.make_async_remote_copy(
            src_ref=scales.at[w, me], dst_ref=scales.at[w, me], send_sem=ag_send.at[w], recv_sem=ag_recv.at[w],
            device_id={"zero": t}, device_id_type=MESH))

    def finish_scales(w):
        got = scales.at[w, pl.ds(0, Z - 1)]
        pltpu.make_async_copy(got, got, ag_recv.at[w]).wait()
        inverse[w] = 1.0 / scales[w]

    def turn(p, piece):
        for h in range(2):
            turned = []
            for b in range(h * half, (h + 1) * half):
                both = [piece(e, b) for e in (2 * p + core, 2 * p + 1 - core)]
                turned.append(jnp.concatenate(both, axis=0).T)
            yield h, jnp.concatenate(turned, axis=0).reshape(Z // 2, own, LANES)

    def narrow(w, p):
        def piece(e, b):
            return held[w, e, :, b * LANES:(b + 1) * LANES] * inverse[w, e, b:b + 1, :]

        for h, t in turn(p, piece):
            send[pl.ds(h * (Z // 2), Z // 2), w * pairs + p] = t.astype(jnp.bfloat16)

    def copy_raw(p):
        for h, t in turn(p, lambda e, b: held[0, e, :, b * LANES:(b + 1) * LANES]):
            raw_send[p, pl.ds(h * (Z // 2), Z // 2)] = t

    def send_raw(i):
        p, at = i // per_pair, pl.ds(8 * (i % per_pair), 8)
        to_plane(lambda t: pltpu.make_async_remote_copy(
            src_ref=raw_send.at[p, t, at], dst_ref=raw_recv.at[p, me, at],
            send_sem=raw_sent.at[i], recv_sem=raw_got.at[i],
            device_id={"zero": t}, device_id_type=MESH))
        raw_recv[p, me, at] = raw_send[p, me, at]

    first_pair = (raw, 0)
    base = (0, (pairs - raw) // chunk[0])

    def span(w, i):
        return first_pair[w] + i * chunk[w]

    def count(w):
        return (pairs - first_pair[w]) // chunk[w]

    def send_chunk(w, i, steps):
        at = pl.ds(w * pairs + span(w, i), chunk[w])
        for s in steps:
            t = stepped(me, s)
            pltpu.make_async_remote_copy(
                src_ref=send.at[t, at], dst_ref=recv.at[me, at], send_sem=bulk_sent, recv_sem=bulk_got.at[base[w] + i],
                device_id={"zero": t}, device_id_type=MESH).start()

    def prepare(w, i):
        for j in range(chunk[w]):
            narrow(w, span(w, i) + j)
        at = pl.ds(w * pairs + span(w, i), chunk[w])
        recv[me, at] = send[me, at]

    for q in range(loads):
        load(1, q).start()
        sums_of(0, q)
    for p in range(raw):
        copy_raw(p)
    pl.semaphore_wait(barrier, Z - 1 + 2)
    scatter_sums(0)

    for copy in small:
        copy.wait()
    low = router_ref[:16, :] * gain_ref[...]
    high = router_ref[16:, :] * gain_ref[...]
    first = jnp.where(core == 0, low, high)
    second = jnp.where(core == 0, high, low)
    router_part[me // 2] = jnp.concatenate([first, second], axis=1).astype(jnp.bfloat16)

    def router_row(k, _):
        t = (((me // 8 + k // 4) % 4) * 4 + (me // 2 + k) % 4) * 2 + core
        pltpu.make_async_remote_copy(
            src_ref=router_part.at[me // 2], dst_ref=router_part.at[me // 2],
            send_sem=rt_send, recv_sem=rt_recv, device_id={"zero": t}, device_id_type=MESH).start()
        return 0

    lax.fori_loop(1, 16, router_row, 0)
    for i in range(tiles[0]):
        send_raw(i)
    for q in range(loads):
        sums_of(1, q)
    scatter_sums(1)
    for i in range(tiles[0], tiles[0] + tiles[1]):
        send_raw(i)
    gather_scales(0)
    for i in range(tiles[0] + tiles[1], sum(tiles)):
        send_raw(i)
    gather_scales(1)

    def rest(ref, t):
        return ref.at[t, raw - 1, pl.ds(own - kept, kept)]

    for w in range(2):
        finish_scales(w)
        if w == 0 and kept:
            narrow(0, raw - 1)
            to_plane(lambda t: pltpu.make_async_remote_copy(
                src_ref=rest(send, t), dst_ref=rest(recv, me), send_sem=rest_sent, recv_sem=rest_got,
                device_id={"zero": t}, device_id_type=MESH))
            recv[me, raw - 1, own - kept:, :] = send[me, raw - 1, own - kept:, :]

        lead = (0, 2)[w]

        def begin(i, _):
            prepare(w, i)
            send_chunk(w, i, STEPS[:FAR])
            return 0

        def both(i, _):
            begin(i + lead, 0)
            send_chunk(w, i, STEPS[FAR:])
            return 0

        def end(i, _):
            send_chunk(w, i, STEPS[FAR:])
            return 0

        if lead:
            lax.fori_loop(0, lead, begin, 0)
        lax.fori_loop(0, count(w) - lead, both, 0)
        if lead:
            lax.fori_loop(count(w) - lead, count(w), end, 0)

    partner = {"zero": (me // 2) * 2 + 1 - core}
    opposite = (bank + 2) % 4

    def pass_on(of_bank, to, sem):
        slot = router_got.at[2 * of_bank + core]
        pltpu.make_async_remote_copy(
            src_ref=slot, dst_ref=slot, send_sem=rx_send.at[sem], recv_sem=rx_recv.at[sem],
            device_id=to, device_id_type=MESH).start()

    def passed_on(count, sem, which):
        got = router_got.at[pl.ds(0, count)]
        pltpu.make_async_copy(got, got, which.at[sem]).wait()

    got = router_part.at[pl.ds(0, 15)]
    pltpu.make_async_copy(got, got, rt_recv).wait()
    router_got[2 * bank + core] = router_part[...]
    pass_on(bank, {"bank": up_bank}, 0)
    pass_on(bank, {"bank": down_bank}, 0)
    pass_on(bank, partner, 0)

    def relay_near():
        passed_on(3, 0, rx_recv)
        pass_on(down_bank, {"bank": up_bank}, 1)
        pass_on(down_bank, partner, 1)
        pass_on(up_bank, partner, 1)

    def relay_far():
        passed_on(3, 1, rx_recv)
        pass_on(opposite, partner, 2)

    for w, o in ((0, out_sgate), (1, out_sup)):
        for b in range(blocks):
            scales_t[b * LANES:(b + 1) * LANES, :] = scales[w, :, b, :].T
        o[...] = scales_t[pl.ds(pl.multiple_of(me * own, 8), own), :]

    low_lanes = lax.broadcasted_iota(jnp.int32, (own, LANES), 1) < LANES // 2

    def merge(out, g, p):
        for k in range(Z // 2):
            a = recv[2 * k, g].astype(jnp.float32)
            b = recv[2 * k + 1, g].astype(jnp.float32)
            at = slice(k * LANES, (k + 1) * LANES)
            out[2 * p, :, at] = jnp.where(low_lanes, a, b).astype(jnp.bfloat16)
            out[2 * p + 1, :, at] = pltpu.roll(jnp.where(low_lanes, b, a), LANES // 2, 1).astype(jnp.bfloat16)

    def take(w, out, start, stop):
        def body(i, _):
            got = recv.at[pl.ds(0, Z - 1), pl.ds(w * pairs + span(w, i), chunk[w])]
            pltpu.make_async_copy(got, got, bulk_got.at[base[w] + i]).wait()
            for j in range(chunk[w]):
                merge(out, w * pairs + span(w, i) + j, span(w, i) + j)
            return 0

        lax.fori_loop(start, stop, body, 0)

    for i in range(sum(tiles)):
        at = pl.ds(8 * (i % per_pair), 8)
        got = raw_recv.at[i // per_pair, pl.ds(0, Z - 1), at]
        pltpu.make_async_copy(got, got, raw_got.at[i]).wait()
    if kept:
        got = rest(recv, pl.ds(0, Z - 1))
        pltpu.make_async_copy(got, got, rest_got).wait()
    for p in range(raw):
        even = 1.0 / out_sgate[:, 2 * p:2 * p + 1]
        odd = 1.0 / out_sgate[:, 2 * p + 1:2 * p + 2]
        for k in range(Z // 2):
            a = raw_recv[p, 2 * k]
            b = raw_recv[p, 2 * k + 1]
            at = slice(k * LANES, (k + 1) * LANES)
            one = jnp.where(low_lanes, a, b) * even
            other = pltpu.roll(jnp.where(low_lanes, b, a), LANES // 2, 1) * odd
            if p == raw - 1 and kept:
                a = recv[2 * k, p].astype(jnp.float32)
                b = recv[2 * k + 1, p].astype(jnp.float32)
                is_raw = lax.broadcasted_iota(jnp.int32, (own, LANES), 0) < own - kept
                one = jnp.where(is_raw, one, jnp.where(low_lanes, a, b))
                other = jnp.where(is_raw, other, pltpu.roll(jnp.where(low_lanes, b, a), LANES // 2, 1))
            out_gate[2 * p, :, at] = one.astype(jnp.bfloat16)
            out_gate[2 * p + 1, :, at] = other.astype(jnp.bfloat16)

    take(0, out_gate, 0, count(0) // 3)
    relay_near()
    take(0, out_gate, count(0) // 3, 2 * (count(0) // 3))
    relay_far()
    take(0, out_gate, 2 * (count(0) // 3), count(0))

    passed_on(1, 2, rx_recv)
    low_r = lax.broadcasted_iota(jnp.int32, (16, LANES), 1) < LANES // 2

    def router_rows(k, _):
        pieces = []
        for z in range(4):
            a = router_got[2 * z, k].astype(jnp.float32)
            b = router_got[2 * z + 1, k].astype(jnp.float32)
            pieces.append(jnp.where(low_r, a, b))
            pieces.append(pltpu.roll(jnp.where(low_r, b, a), LANES // 2, 1))
        out_router[pl.ds(pl.multiple_of(k * LANES, LANES), LANES), :] = (
            jnp.concatenate(pieces, axis=0).T.astype(jnp.bfloat16))
        return 0

    lax.fori_loop(0, 16, router_rows, 0)

    take(1, out_up, 0, count(1))

    for w in range(2):
        left = sums.at[w, pl.ds(0, Z - 1)]
        pltpu.make_async_copy(left, left, rs_send.at[w]).wait()
        pltpu.make_async_copy(left, left, ag_send.at[w]).wait()
    for i in range(sum(tiles)):
        left = raw_send.at[i // per_pair, pl.ds(0, Z - 1), pl.ds(8 * (i % per_pair), 8)]
        pltpu.make_async_copy(left, left, raw_sent.at[i]).wait()
    if kept:
        left = rest(send, pl.ds(0, Z - 1))
        pltpu.make_async_copy(left, left, rest_sent).wait()
    left = send.at[pl.ds(0, Z - 1), pl.ds(raw, 2 * pairs - raw)]
    pltpu.make_async_copy(left, left, bulk_sent).wait()
    left = router_part.at[pl.ds(0, 15)]
    pltpu.make_async_copy(left, left, rt_send).wait()
    for sem, sent in ((0, 3), (1, 3), (2, 1)):
        passed_on(sent, sem, rx_send)


def write_out(*refs):
    n = 5
    ins, outs, sem = refs[:n], refs[n:2 * n], refs[2 * n]
    copies = []
    for i in range(n):
        copy = pltpu.make_async_copy(ins[i], outs[i], sem.at[i])
        copy.start()
        copies.append(copy)
    for copy in copies:
        copy.wait()


def shards(w_gate, w_up, router_weight, router_gain):
    experts, rows, cols = w_gate.shape
    own = cols // Z
    tiles = (1, 1, 2)
    raw = -(-sum(tiles) // (own // 8))
    chunk = (1, 1)
    pairs = experts // 2
    chunks = (pairs - raw) // chunk[0] + pairs // chunk[1]
    f32, bf16 = jnp.float32, jnp.bfloat16
    dma = pltpu.SemaphoreType.DMA
    hbm = pl.BlockSpec(memory_space=pltpu.HBM)
    vmem = pl.BlockSpec(memory_space=pltpu.VMEM)
    shapes = [
        ((experts, own, Z * rows), bf16), ((experts, own, Z * rows), bf16),
        ((own, experts), f32), ((own, experts), f32), ((Z * rows, LANES), bf16),
    ]
    moved = pl.pallas_call(
        functools.partial(exchange, experts, rows, cols, tiles, chunk),
        out_shape=[pltpu.VMEM(s, d) for s, d in shapes],
        in_specs=[hbm] * 4,
        out_specs=[vmem] * 5,
        scratch_shapes=[
            pltpu.VMEM((2, experts, rows, cols), f32),
            pltpu.VMEM((2, experts, cols // LANES, LANES), f32),
            pltpu.VMEM((2, Z, cols // LANES, LANES), f32),
            pltpu.VMEM((2, experts, cols // LANES, LANES), f32),
            pltpu.VMEM((2, experts, cols // LANES, LANES), f32),
            pltpu.VMEM((cols, experts), f32),
            pltpu.VMEM((Z, 2 * pairs, own, LANES), bf16),
            pltpu.VMEM((Z, 2 * pairs, own, LANES), bf16),
            pltpu.VMEM((raw, Z, own, LANES), f32),
            pltpu.VMEM((raw, Z, own, LANES), f32),
            pltpu.VMEM((experts, rows), f32),
            pltpu.VMEM((1, rows), f32),
            pltpu.VMEM((16, 16, LANES), bf16),
            pltpu.VMEM((8, 16, 16, LANES), bf16),
            dma((2,)), dma((8,)), dma((2,)), dma((2,)), dma((2,)), dma((2,)), dma, dma((chunks,)),
            dma((sum(tiles),)), dma((sum(tiles),)), dma, dma,
            dma, dma, dma((3,)), dma((3,)),
        ],
        compiler_params=pltpu.CompilerParams(
            collective_id=0, has_side_effects=True, vmem_limit_bytes=54 << 20),
    )(w_gate, w_up, router_weight.T, router_gain[None, :])
    outs = pl.pallas_call(
        write_out,
        out_shape=[jax.ShapeDtypeStruct(s, d) for s, d in shapes],
        in_specs=[pl.BlockSpec(memory_space=pl.ANY)] * 5,
        out_specs=[hbm] * 5,
        scratch_shapes=[dma((5,))],
        compiler_params=pltpu.CompilerParams(vmem_limit_bytes=1 << 20),
    )(*moved)
    gate, up, sgate, sup, router = outs
    return (gate.transpose(0, 2, 1), up.transpose(0, 2, 1), sgate.T, sup.T, router)


def solution(mesh):
    placed = (P("bank", "zero", None), P("bank", "zero", None), P("zero", "bank"), P("zero"))
    return jax.shard_map(
        shards,
        mesh=mesh,
        in_specs=placed,
        out_specs=(
            P("bank", None, "zero"),
            P("bank", None, "zero"),
            P("bank", "zero"),
            P("bank", "zero"),
            P(),
        ),
        check_vma=False,
    )
```

```python
import functools

import jax
import jax.numpy as jnp
from jax import lax
from jax.experimental import pallas as pl
from jax.experimental.pallas import tpu as pltpu
from jax.sharding import PartitionSpec as P

MESH = pl.DeviceIdType.MESH
Z = 32
LANES = 128


STEPS = sorted(
    ((dy, dx, dc) for dy in range(4) for dx in range(4) for dc in range(2) if dy or dx or dc),
    key=lambda s: (-(min(s[0], 4 - s[0]) + min(s[1], 4 - s[1])), -s[2], (s[0] - s[1]) % 4, -s[0]),
)


FAR = 22


def stepped(me, step):
    y, x, c = me // 8, (me // 2) % 4, me % 2
    return (((y + step[0]) % 4) * 4 + (x + step[1]) % 4) * 2 + (c + step[2]) % 2


def exchange(
    experts, rows, cols, tiles, chunk,
    gate_hbm, up_hbm, router_hbm, gain_hbm,
    out_gate, out_up, out_sgate, out_sup, out_router,
    held, sums, parts, scales, inverse, scales_t, send, recv, raw_send, raw_recv, router_ref, gain_ref, router_part, router_got,
    small_sem, load_sem, rs_send, rs_recv, ag_send, ag_recv, bulk_sent, bulk_got,
    raw_sent, raw_got, rest_sent, rest_got,
    rt_send, rt_recv, rx_send, rx_recv,
):
    bank = lax.axis_index("bank")
    me = lax.axis_index("zero")
    core = me % 2
    blocks = cols // LANES
    own = cols // Z
    pairs = experts // 2
    half = blocks // 2
    per_pair = own // 8
    raw = -(-sum(tiles) // per_pair)
    kept = own - 8 * (sum(tiles) - (raw - 1) * per_pair)
    weights = (gate_hbm, up_hbm)
    loads = 4
    step = experts // loads

    def load(w, q):
        at = pl.ds(q * step, step)
        return pltpu.make_async_copy(weights[w].at[at], held.at[w, at], load_sem.at[w * loads + q])

    barrier = pltpu.get_barrier_semaphore()
    for s in STEPS:
        pl.semaphore_signal(barrier, inc=1, device_id={"zero": stepped(me, s)}, device_id_type=MESH)
    up_bank, down_bank = (bank + 1) % 4, (bank + 3) % 4
    for other in (up_bank, down_bank):
        pl.semaphore_signal(barrier, inc=1, device_id={"bank": other}, device_id_type=MESH)

    for q in range(loads):
        load(0, q).start()
    small = [
        pltpu.make_async_copy(router_hbm, router_ref, small_sem.at[0]),
        pltpu.make_async_copy(gain_hbm, gain_ref, small_sem.at[1]),
    ]
    for copy in small:
        copy.start()

    def sums_of(w, q):
        load(w, q).wait()

        def body(e, _):
            for b in range(blocks):
                x = held[w, e, :, b * LANES:(b + 1) * LANES]
                sums[w, e, b:b + 1, :] = jnp.sum(x * x, axis=0, keepdims=True)
            return 0

        lax.fori_loop(q * step, (q + 1) * step, body, 0)

    def to_plane(make):
        for s in STEPS:
            make(stepped(me, s)).start()

    def scatter_sums(w):
        to_plane(lambda t: pltpu.make_async_remote_copy(
            src_ref=sums.at[w, t], dst_ref=parts.at[w, me], send_sem=rs_send.at[w], recv_sem=rs_recv.at[w],
            device_id={"zero": t}, device_id_type=MESH))
        parts[w, me] = sums[w, me]

    def gather_scales(w):
        got = parts.at[w, pl.ds(0, Z - 1)]
        pltpu.make_async_copy(got, got, rs_recv.at[w]).wait()
        scales[w, me] = jnp.sqrt(jnp.sum(parts[w], axis=0))
        to_plane(lambda t: pltpu.make_async_remote_copy(
            src_ref=scales.at[w, me], dst_ref=scales.at[w, me], send_sem=ag_send.at[w], recv_sem=ag_recv.at[w],
            device_id={"zero": t}, device_id_type=MESH))

    def finish_scales(w):
        got = scales.at[w, pl.ds(0, Z - 1)]
        pltpu.make_async_copy(got, got, ag_recv.at[w]).wait()
        inverse[w] = 1.0 / scales[w]

    def turn(p, piece):
        for h in range(2):
            turned = []
            for b in range(h * half, (h + 1) * half):
                both = [piece(e, b) for e in (2 * p + core, 2 * p + 1 - core)]
                turned.append(jnp.concatenate(both, axis=0).T)
            yield h, jnp.concatenate(turned, axis=0).reshape(Z // 2, own, LANES)

    def narrow(w, p):
        def piece(e, b):
            return held[w, e, :, b * LANES:(b + 1) * LANES] * inverse[w, e, b:b + 1, :]

        for h, t in turn(p, piece):
            send[pl.ds(h * (Z // 2), Z // 2), w * pairs + p] = t.astype(jnp.bfloat16)

    def copy_raw(p):
        for h, t in turn(p, lambda e, b: held[0, e, :, b * LANES:(b + 1) * LANES]):
            raw_send[p, pl.ds(h * (Z // 2), Z // 2)] = t

    def send_raw(i):
        p, at = i // per_pair, pl.ds(8 * (i % per_pair), 8)
        to_plane(lambda t: pltpu.make_async_remote_copy(
            src_ref=raw_send.at[p, t, at], dst_ref=raw_recv.at[p, me, at],
            send_sem=raw_sent.at[i], recv_sem=raw_got.at[i],
            device_id={"zero": t}, device_id_type=MESH))
        raw_recv[p, me, at] = raw_send[p, me, at]

    first_pair = (raw, 0)
    base = (0, (pairs - raw) // chunk[0])

    def span(w, i):
        return first_pair[w] + i * chunk[w]

    def count(w):
        return (pairs - first_pair[w]) // chunk[w]

    def send_chunk(w, i, steps):
        at = pl.ds(w * pairs + span(w, i), chunk[w])
        for s in steps:
            t = stepped(me, s)
            pltpu.make_async_remote_copy(
                src_ref=send.at[t, at], dst_ref=recv.at[me, at], send_sem=bulk_sent, recv_sem=bulk_got.at[base[w] + i],
                device_id={"zero": t}, device_id_type=MESH).start()

    def prepare(w, i):
        for j in range(chunk[w]):
            narrow(w, span(w, i) + j)
        at = pl.ds(w * pairs + span(w, i), chunk[w])
        recv[me, at] = send[me, at]

    for q in range(loads):
        load(1, q).start()
        sums_of(0, q)
    for p in range(raw):
        copy_raw(p)
    pl.semaphore_wait(barrier, Z - 1 + 2)
    scatter_sums(0)

    for copy in small:
        copy.wait()
    low = router_ref[:16, :] * gain_ref[...]
    high = router_ref[16:, :] * gain_ref[...]
    first = jnp.where(core == 0, low, high)
    second = jnp.where(core == 0, high, low)
    router_part[me // 2] = jnp.concatenate([first, second], axis=1).astype(jnp.bfloat16)

    def router_row(k, _):
        t = (((me // 8 + k // 4) % 4) * 4 + (me // 2 + k) % 4) * 2 + core
        pltpu.make_async_remote_copy(
            src_ref=router_part.at[me // 2], dst_ref=router_part.at[me // 2],
            send_sem=rt_send, recv_sem=rt_recv, device_id={"zero": t}, device_id_type=MESH).start()
        return 0

    lax.fori_loop(1, 16, router_row, 0)
    for i in range(tiles[0]):
        send_raw(i)
    for q in range(loads):
        sums_of(1, q)
    scatter_sums(1)
    for i in range(tiles[0], tiles[0] + tiles[1]):
        send_raw(i)
    gather_scales(0)
    for i in range(tiles[0] + tiles[1], sum(tiles)):
        send_raw(i)
    gather_scales(1)

    def rest(ref, t):
        return ref.at[t, raw - 1, pl.ds(own - kept, kept)]

    for w in range(2):
        finish_scales(w)
        if w == 0 and kept:
            narrow(0, raw - 1)
            to_plane(lambda t: pltpu.make_async_remote_copy(
                src_ref=rest(send, t), dst_ref=rest(recv, me), send_sem=rest_sent, recv_sem=rest_got,
                device_id={"zero": t}, device_id_type=MESH))
            recv[me, raw - 1, own - kept:, :] = send[me, raw - 1, own - kept:, :]

        lead = (0, 2)[w]

        def begin(i, _):
            prepare(w, i)
            send_chunk(w, i, STEPS[:FAR])
            return 0

        def both(i, _):
            begin(i + lead, 0)
            send_chunk(w, i, STEPS[FAR:])
            return 0

        def end(i, _):
            send_chunk(w, i, STEPS[FAR:])
            return 0

        if lead:
            lax.fori_loop(0, lead, begin, 0)
        lax.fori_loop(0, count(w) - lead, both, 0)
        if lead:
            lax.fori_loop(count(w) - lead, count(w), end, 0)

    partner = {"zero": (me // 2) * 2 + 1 - core}
    opposite = (bank + 2) % 4

    def pass_on(of_bank, to, sem):
        slot = router_got.at[2 * of_bank + core]
        pltpu.make_async_remote_copy(
            src_ref=slot, dst_ref=slot, send_sem=rx_send.at[sem], recv_sem=rx_recv.at[sem],
            device_id=to, device_id_type=MESH).start()

    def passed_on(count, sem, which):
        got = router_got.at[pl.ds(0, count)]
        pltpu.make_async_copy(got, got, which.at[sem]).wait()

    got = router_part.at[pl.ds(0, 15)]
    pltpu.make_async_copy(got, got, rt_recv).wait()
    router_got[2 * bank + core] = router_part[...]
    pass_on(bank, {"bank": up_bank}, 0)
    pass_on(bank, {"bank": down_bank}, 0)
    pass_on(bank, partner, 0)

    def relay_near():
        passed_on(3, 0, rx_recv)
        pass_on(down_bank, {"bank": up_bank}, 1)
        pass_on(down_bank, partner, 1)
        pass_on(up_bank, partner, 1)

    def relay_far():
        passed_on(3, 1, rx_recv)
        pass_on(opposite, partner, 2)

    for w, o in ((0, out_sgate), (1, out_sup)):
        for b in range(blocks):
            scales_t[b * LANES:(b + 1) * LANES, :] = scales[w, :, b, :].T
        o[...] = scales_t[pl.ds(pl.multiple_of(me * own, 8), own), :]

    low_lanes = lax.broadcasted_iota(jnp.int32, (own, LANES), 1) < LANES // 2

    def merge(out, g, p):
        for k in range(Z // 2):
            a = recv[2 * k, g].astype(jnp.float32)
            b = recv[2 * k + 1, g].astype(jnp.float32)
            at = slice(k * LANES, (k + 1) * LANES)
            out[2 * p, :, at] = jnp.where(low_lanes, a, b).astype(jnp.bfloat16)
            out[2 * p + 1, :, at] = pltpu.roll(jnp.where(low_lanes, b, a), LANES // 2, 1).astype(jnp.bfloat16)

    def take(w, out, start, stop):
        def body(i, _):
            got = recv.at[pl.ds(0, Z - 1), pl.ds(w * pairs + span(w, i), chunk[w])]
            pltpu.make_async_copy(got, got, bulk_got.at[base[w] + i]).wait()
            for j in range(chunk[w]):
                merge(out, w * pairs + span(w, i) + j, span(w, i) + j)
            return 0

        lax.fori_loop(start, stop, body, 0)

    for i in range(sum(tiles)):
        at = pl.ds(8 * (i % per_pair), 8)
        got = raw_recv.at[i // per_pair, pl.ds(0, Z - 1), at]
        pltpu.make_async_copy(got, got, raw_got.at[i]).wait()
    if kept:
        got = rest(recv, pl.ds(0, Z - 1))
        pltpu.make_async_copy(got, got, rest_got).wait()
    for p in range(raw):
        even = 1.0 / out_sgate[:, 2 * p:2 * p + 1]
        odd = 1.0 / out_sgate[:, 2 * p + 1:2 * p + 2]
        for k in range(Z // 2):
            a = raw_recv[p, 2 * k]
            b = raw_recv[p, 2 * k + 1]
            at = slice(k * LANES, (k + 1) * LANES)
            one = jnp.where(low_lanes, a, b) * even
            other = pltpu.roll(jnp.where(low_lanes, b, a), LANES // 2, 1) * odd
            if p == raw - 1 and kept:
                a = recv[2 * k, p].astype(jnp.float32)
                b = recv[2 * k + 1, p].astype(jnp.float32)
                is_raw = lax.broadcasted_iota(jnp.int32, (own, LANES), 0) < own - kept
                one = jnp.where(is_raw, one, jnp.where(low_lanes, a, b))
                other = jnp.where(is_raw, other, pltpu.roll(jnp.where(low_lanes, b, a), LANES // 2, 1))
            out_gate[2 * p, :, at] = one.astype(jnp.bfloat16)
            out_gate[2 * p + 1, :, at] = other.astype(jnp.bfloat16)

    take(0, out_gate, 0, count(0) // 3)
    relay_near()
    take(0, out_gate, count(0) // 3, 2 * (count(0) // 3))
    relay_far()
    take(0, out_gate, 2 * (count(0) // 3), count(0))

    passed_on(1, 2, rx_recv)
    low_r = lax.broadcasted_iota(jnp.int32, (16, LANES), 1) < LANES // 2

    def router_rows(k, _):
        pieces = []
        for z in range(4):
            a = router_got[2 * z, k].astype(jnp.float32)
            b = router_got[2 * z + 1, k].astype(jnp.float32)
            pieces.append(jnp.where(low_r, a, b))
            pieces.append(pltpu.roll(jnp.where(low_r, b, a), LANES // 2, 1))
        out_router[pl.ds(pl.multiple_of(k * LANES, LANES), LANES), :] = (
            jnp.concatenate(pieces, axis=0).T.astype(jnp.bfloat16))
        return 0

    lax.fori_loop(0, 16, router_rows, 0)

    take(1, out_up, 0, count(1))

    for w in range(2):
        left = sums.at[w, pl.ds(0, Z - 1)]
        pltpu.make_async_copy(left, left, rs_send.at[w]).wait()
        pltpu.make_async_copy(left, left, ag_send.at[w]).wait()
    for i in range(sum(tiles)):
        left = raw_send.at[i // per_pair, pl.ds(0, Z - 1), pl.ds(8 * (i % per_pair), 8)]
        pltpu.make_async_copy(left, left, raw_sent.at[i]).wait()
    if kept:
        left = rest(send, pl.ds(0, Z - 1))
        pltpu.make_async_copy(left, left, rest_sent).wait()
    left = send.at[pl.ds(0, Z - 1), pl.ds(raw, 2 * pairs - raw)]
    pltpu.make_async_copy(left, left, bulk_sent).wait()
    left = router_part.at[pl.ds(0, 15)]
    pltpu.make_async_copy(left, left, rt_send).wait()
    for sem, sent in ((0, 3), (1, 3), (2, 1)):
        passed_on(sent, sem, rx_send)


def write_out(*refs):
    n = 5
    ins, outs, sem = refs[:n], refs[n:2 * n], refs[2 * n]
    copies = []
    for i in range(n):
        copy = pltpu.make_async_copy(ins[i], outs[i], sem.at[i])
        copy.start()
        copies.append(copy)
    for copy in copies:
        copy.wait()


def shards(w_gate, w_up, router_weight, router_gain):
    experts, rows, cols = w_gate.shape
    own = cols // Z
    tiles = (1, 1, 2)
    raw = -(-sum(tiles) // (own // 8))
    chunk = (2, 2)
    pairs = experts // 2
    chunks = (pairs - raw) // chunk[0] + pairs // chunk[1]
    f32, bf16 = jnp.float32, jnp.bfloat16
    dma = pltpu.SemaphoreType.DMA
    hbm = pl.BlockSpec(memory_space=pltpu.HBM)
    vmem = pl.BlockSpec(memory_space=pltpu.VMEM)
    shapes = [
        ((experts, own, Z * rows), bf16), ((experts, own, Z * rows), bf16),
        ((own, experts), f32), ((own, experts), f32), ((Z * rows, LANES), bf16),
    ]
    moved = pl.pallas_call(
        functools.partial(exchange, experts, rows, cols, tiles, chunk),
        out_shape=[pltpu.VMEM(s, d) for s, d in shapes],
        in_specs=[hbm] * 4,
        out_specs=[vmem] * 5,
        scratch_shapes=[
            pltpu.VMEM((2, experts, rows, cols), f32),
            pltpu.VMEM((2, experts, cols // LANES, LANES), f32),
            pltpu.VMEM((2, Z, cols // LANES, LANES), f32),
            pltpu.VMEM((2, experts, cols // LANES, LANES), f32),
            pltpu.VMEM((2, experts, cols // LANES, LANES), f32),
            pltpu.VMEM((cols, experts), f32),
            pltpu.VMEM((Z, 2 * pairs, own, LANES), bf16),
            pltpu.VMEM((Z, 2 * pairs, own, LANES), bf16),
            pltpu.VMEM((raw, Z, own, LANES), f32),
            pltpu.VMEM((raw, Z, own, LANES), f32),
            pltpu.VMEM((experts, rows), f32),
            pltpu.VMEM((1, rows), f32),
            pltpu.VMEM((16, 16, LANES), bf16),
            pltpu.VMEM((8, 16, 16, LANES), bf16),
            dma((2,)), dma((8,)), dma((2,)), dma((2,)), dma((2,)), dma((2,)), dma, dma((chunks,)),
            dma((sum(tiles),)), dma((sum(tiles),)), dma, dma,
            dma, dma, dma((3,)), dma((3,)),
        ],
        compiler_params=pltpu.CompilerParams(
            collective_id=0, has_side_effects=True, vmem_limit_bytes=54 << 20),
    )(w_gate, w_up, router_weight.T, router_gain[None, :])
    outs = pl.pallas_call(
        write_out,
        out_shape=[jax.ShapeDtypeStruct(s, d) for s, d in shapes],
        in_specs=[pl.BlockSpec(memory_space=pl.ANY)] * 5,
        out_specs=[hbm] * 5,
        scratch_shapes=[dma((5,))],
        compiler_params=pltpu.CompilerParams(vmem_limit_bytes=1 << 20),
    )(*moved)
    gate, up, sgate, sup, router = outs
    return (gate.transpose(0, 2, 1), up.transpose(0, 2, 1), sgate.T, sup.T, router)


def solution(mesh):
    placed = (P("bank", "zero", None), P("bank", "zero", None), P("zero", "bank"), P("zero"))
    return jax.shard_map(
        shards,
        mesh=mesh,
        in_specs=placed,
        out_specs=(
            P("bank", None, "zero"),
            P("bank", None, "zero"),
            P("bank", "zero"),
            P("bank", "zero"),
            P(),
        ),
        check_vma=False,
    )
```
